32 devices in a mesh: strata: 8 (over z, x), users: 4 (over y, core).
Axes of the slice: x: 2, y: 2, z: 4, core: 2. Of those that a mesh axis runs over, the one named last changes fastest.
Arguments:
- user_factors: float32 [65536, 256], P(('strata', 'users')), may hold values from -1.5 to 1.5
- item_factors: float32 [8192, 256], P(('strata', 'users')), may hold values from -1.5 to 1.5
- tile_rows: int32 [8, 4, 2, 64], P('strata', 'users'), may hold values from 0 to 15, as said below
- tile_columns: int32 [8, 4, 2, 64], P('strata', 'users'), may hold values from 0 to 7, as said below
- tile_counts: int32 [8, 4, 2], P('strata', 'users'), may hold values from 8 to 64, as said below
- ratings: int32 [8, 4, 2, 64, 128, 128], P('strata', 'users'), may hold values from 0 to 5
Outputs:
- updated_users: float32 [65536, 256], P(('strata', 'users'))
- updated_items: float32 [8192, 256], P(('strata', 'users'))
The draws below stay inside these ranges and needn't reach their ends.
Inputs may be any that keep to these rules, and one draw needn't show every extreme that they name: `tile_rows`: row tile of each slot within the device's users. `tile_columns`: item tile of each slot within the step's item block; a device's slots of one step name distinct pairs of user tile and item tile, padding slots included. `tile_counts`: in every step some device uses all 64 slots.
All inputs are finite; a program needn't handle non-finite values.
Results may differ from the reference program's by a relative error of at most 0.0004.
Values may be sent and summed in bfloat16 or wider, within the bound.
No kernel may reach another device: no remote copies, remote signals or barrier semaphores. Data moves between devices by JAX's collectives and lax.ppermute only.
A program may use at most 128 MiB of HBM per device.

```python
import jax
import jax.numpy as jnp
from jax import lax

K = 256
TILE = 128
ITEM_TILES = 8
ROW_TILES = 16
MAXT = 64
STEPS = 2
STRATA = 8
SHARDS = 4
USERS_ALL = 65536
ITEMS = 8192


def tile_lists(key):
    key = jax.random.fold_in(key, 7)
    keys = jax.random.split(key, STRATA * SHARDS * STEPS)
    cells = ROW_TILES * ITEM_TILES
    picks = jax.vmap(lambda single: jax.random.permutation(single, cells)[:MAXT])(keys)
    picks = picks.reshape(STRATA, SHARDS, STEPS, MAXT).astype(jnp.int32)
    return (picks // ITEM_TILES, picks % ITEM_TILES)


def draw_tile_rows(key, part):
    return tile_lists(key)[0]


def draw_tile_columns(key, part):
    return tile_lists(key)[1]


def draw_tile_counts(key, part):
    lowest = max(MAXT // 8, 1)
    spread = MAXT - lowest
    first_key, second_key, third_key = jax.random.split(jax.random.fold_in(key, 11), 3)
    first = jax.random.randint(first_key, (STRATA, SHARDS, STEPS), 0, spread + 1)
    second = jax.random.randint(second_key, (STRATA, SHARDS, STEPS), 0, spread + 1)
    counts = lowest + first * second // max(spread, 1)
    chosen = jax.random.randint(third_key, (STEPS,), 0, STRATA * SHARDS)
    fullest = (jnp.arange(STRATA * SHARDS)[:, None] == chosen[None, :]).reshape(STRATA, SHARDS, STEPS)
    return jnp.where(fullest, MAXT, counts).astype(jnp.int32)


def draw_ratings(key, part):
    first_key, second_key = jax.random.split(jax.random.fold_in(key, 13))
    density = jax.random.randint(first_key, (STRATA, SHARDS, STEPS, MAXT, 1, 1), 10, 61)
    raw = jax.random.randint(second_key, (STRATA, SHARDS, STEPS, MAXT, TILE, TILE), 0, 500)
    return jnp.where(raw % 100 < density, raw // 100 + 1, 0).astype(jnp.int32)


def steps_of(stream_key, extent, pieces, low, largest):
    factor_of = 1.0
    for position, blocks in pieces:
        draws = jax.random.uniform(jax.random.fold_in(jax.random.fold_in(stream_key, 6), position), (blocks,), jnp.float32, low / len(pieces), largest / len(pieces))
        factor_of = factor_of * jnp.repeat(jnp.exp(draws), extent[position] // blocks).reshape((-1,) + (1,) * (len(extent) - 1 - position))
    return factor_of


def centred(rng, dims, deviation, bound, cuts=(), held_as=jnp.bfloat16):
    gain = steps_of(rng, dims, cuts, -0.22, 0.18) if cuts else 1.0
    values = jax.random.normal(rng, dims, jnp.float32) * deviation * gain
    return jnp.minimum(jnp.maximum(values, -bound), bound).astype(held_as)


def setup_inputs(seed: int = 0) -> dict:
    key_of = jax.random.split(jax.random.key(seed), 7)
    user_factors = centred(key_of[0], (USERS_ALL, K), 0.25, 1.5, ((0, 32),), jnp.float32)
    item_factors = centred(key_of[1], (ITEMS, K), 0.25, 1.5, ((0, 32),), jnp.float32)
    tile_rows = draw_tile_rows(jax.random.fold_in(key_of[6], 71), 0)
    tile_columns = draw_tile_columns(jax.random.fold_in(key_of[6], 71), 0)
    tile_counts = draw_tile_counts(jax.random.fold_in(key_of[6], 71), 0)
    ratings = draw_ratings(jax.random.fold_in(key_of[6], 71), 0)
    return dict(user_factors=user_factors, item_factors=item_factors, tile_rows=tile_rows, tile_columns=tile_columns, tile_counts=tile_counts, ratings=ratings)


def shard_terms(user_low, block_low, row_blocks, column_blocks, count, rating_tiles):
    user_tiles = user_low[row_blocks].astype(jnp.float32)
    item_tiles = block_low[column_blocks].astype(jnp.float32)
    predicted = jnp.einsum('mik,mjk->mij', user_tiles, item_tiles)
    in_list = jnp.arange(MAXT) < count
    observed = (rating_tiles > 0) & in_list[:, None, None]
    residual = jnp.where(observed, rating_tiles.astype(jnp.float32) - predicted, 0.0).astype(jnp.bfloat16)
    residual = lax.optimization_barrier(residual).astype(jnp.float32)
    user_terms = jnp.einsum('mij,mjk->mik', residual, item_tiles)
    item_terms = jnp.einsum('mij,mik->mjk', residual, user_tiles)
    user_grad = jnp.zeros((ROW_TILES, TILE, K), jnp.float32).at[row_blocks].add(user_terms)
    item_grad = jnp.zeros((ITEM_TILES, TILE, K), jnp.float32).at[column_blocks].add(item_terms)
    return user_grad, item_grad


def stratum_terms(inputs):
    user_low, block_low, row_blocks, column_blocks, counts, rating_tiles = inputs
    user_grad, item_grad = jax.vmap(shard_terms, in_axes=(0, None, 0, 0, 0, 0))(
        user_low, block_low, row_blocks, column_blocks, counts, rating_tiles)
    return user_grad, jnp.sum(item_grad, axis=0)


def reference(user_factors, item_factors, tile_rows, tile_columns, tile_counts, ratings):
    users_now = user_factors
    items_now = item_factors
    for step_index in range(STEPS):
        user_low = users_now.astype(jnp.bfloat16).reshape(STRATA, SHARDS, ROW_TILES, TILE, K)
        item_low = items_now.astype(jnp.bfloat16).reshape(STRATA, ITEM_TILES, TILE, K)
        block_now = jnp.roll(item_low, step_index, axis=0)
        user_grad, item_grad = lax.map(stratum_terms, (
            user_low, block_now, tile_rows[:, :, step_index], tile_columns[:, :, step_index],
            tile_counts[:, :, step_index], ratings[:, :, step_index]))
        user_grad = user_grad.reshape(USERS_ALL, K)
        item_grad = jnp.roll(item_grad, -step_index, axis=0).reshape(ITEMS, K)
        users_now = users_now + 0.01 * (user_grad - 0.05 * users_now)
        items_now = items_now + 0.003 * (item_grad - 0.05 * items_now)
    blocks = items_now.reshape(STRATA, ITEM_TILES * TILE, K)
    return users_now, jnp.roll(blocks, STEPS - 1, axis=0).reshape(ITEMS, K)
```

```python
import functools

import jax
import jax.numpy as jnp
from jax import lax
from jax.experimental import pallas as pl
from jax.experimental.pallas import tpu as pltpu
from jax.sharding import PartitionSpec as P

F32 = jnp.float32
BF16 = jnp.bfloat16
VMEM = pl.BlockSpec(memory_space=pltpu.VMEM)
SMEM = pl.BlockSpec(memory_space=pltpu.SMEM)
ANY = pl.BlockSpec(memory_space=pl.ANY)
BOTH_ROWS = (((0,), (0,)), ((), ()))
BOTH_COLUMNS = (((1,), (1,)), ((), ()))
MIB = 1 << 20


def route(block, strata_shift, users_flip):
    strata, users = lax.axis_size("strata"), lax.axis_size("users")
    pairs = [
        (s * users + u, ((s + strata_shift) % strata) * users + (u ^ users_flip))
        for s in range(strata)
        for u in range(users)
    ]
    return lax.ppermute(block, ("strata", "users"), pairs)


def dense_kernel(step, tiles_per_shard, rows_ref, columns_ref, counts_ref, ratings_ref, dense_ref, tiles, arrived):
    count = counts_ref[0, 0, step]
    flip = lax.axis_index("users") * tiles_per_shard
    tile = tiles.shape[1]

    def copy(m):
        return pltpu.make_async_copy(ratings_ref.at[0, 0, step, m], tiles.at[m], arrived.at[m])

    @pl.loop(0, count)
    def _(m):
        copy(m).start()

    @pl.loop(0, dense_ref.shape[0])
    def _(j):
        @pl.loop(0, dense_ref.shape[1] // tile)
        def _(r):
            dense_ref[j, pl.ds(r * tile, tile), :] = jnp.zeros((tile, tile), BF16)

    @pl.loop(0, count)
    def _(m):
        j = columns_ref[0, 0, step, m] ^ flip
        r = rows_ref[0, 0, step, m]
        copy(m).wait()
        dense_ref[j, pl.ds(pl.multiple_of(r * tile, tile), tile), :] = (
            tiles[m].astype(F32).astype(BF16)
        )


def dense_ratings(step, tiles_per_shard, column_tiles, user_rows, tile_rows, tile_columns, tile_counts, ratings):
    slots, tile = ratings.shape[3], ratings.shape[4]
    return pl.pallas_call(
        functools.partial(dense_kernel, step, tiles_per_shard),
        out_shape=jax.ShapeDtypeStruct((column_tiles, user_rows, tile), BF16),
        in_specs=[SMEM, SMEM, SMEM, ANY],
        out_specs=VMEM,
        scratch_shapes=[
            pltpu.VMEM((slots, tile, tile), jnp.int32),
            pltpu.SemaphoreType.DMA((slots,)),
        ],
        compiler_params=pltpu.CompilerParams(vmem_limit_bytes=12 * MIB),
        cost_estimate=pl.CostEstimate(flops=2 * 10**9, bytes_accessed=8 * MIB, transcendentals=0),
        name=f"dense_{step}",
    )(tile_rows, tile_columns, tile_counts, ratings)


def terms_kernel(columns, chunk, users_ref, dense_ref, *refs):
    number = len(columns)
    item_refs, residual_refs, grad_refs = refs[:number], refs[number : 2 * number], refs[2 * number :]
    tile = item_refs[0].shape[0]
    items = jnp.concatenate([ref[...] for ref in item_refs], axis=0)
    for ref in grad_refs:
        ref[...] = jnp.zeros_like(ref)

    @pl.loop(0, users_ref.shape[0] // chunk)
    def _(i):
        rows = pl.ds(pl.multiple_of(i * chunk, chunk), chunk)
        users = users_ref[rows, :]
        predicted = lax.dot_general(users, items, BOTH_COLUMNS, preferred_element_type=F32)
        for k, j in enumerate(columns):
            rating = dense_ref[j, rows, :].astype(F32)
            residual = jnp.where(
                rating > 0, rating - predicted[:, k * tile : (k + 1) * tile], 0.0
            ).astype(BF16)
            residual_refs[k][rows, :] = residual
            grad_refs[k][...] += lax.dot_general(
                residual, users, BOTH_ROWS, preferred_element_type=F32
            )


def terms(columns, users_low, dense, items):
    user_rows, width = users_low.shape
    tile = items[0].shape[0]
    number = len(columns)
    return pl.pallas_call(
        functools.partial(terms_kernel, columns, min(512, user_rows)),
        out_shape=[jax.ShapeDtypeStruct((user_rows, tile), BF16)] * number
        + [jax.ShapeDtypeStruct((tile, width), F32)] * number,
        in_specs=[VMEM] * (2 + number),
        out_specs=[VMEM] * (2 * number),
        compiler_params=pltpu.CompilerParams(vmem_limit_bytes=16 * MIB),
        cost_estimate=pl.CostEstimate(
            flops=4 * user_rows * tile * width * number, bytes_accessed=MIB, transcendentals=0
        ),
        name="terms_" + "_".join(map(str, columns)),
    )(users_low, dense, *items)


def users_kernel(number, low_out, users_ref, *refs):
    item_refs, residual_refs, outs = refs[:number], refs[number : 2 * number], refs[2 * number :]
    total = None
    for k in range(0, number, 2):
        two = slice(k, k + 2)
        residual = jnp.concatenate([ref[...] for ref in residual_refs[two]], axis=1)
        items = jnp.concatenate([ref[...] for ref in item_refs[two]], axis=0)
        part = jnp.dot(residual, items, preferred_element_type=F32)
        total = part if total is None else total + part
    users = users_ref[...]
    updated = users + 0.01 * (total - 0.05 * users)
    outs[0][...] = updated
    if low_out:
        outs[1][...] = updated.astype(BF16)


def update_users(users, items, residuals, low_out):
    user_rows, width = users.shape
    number = len(items)
    tile = items[0].shape[0]
    chunk = min(256, user_rows)
    block = pl.BlockSpec((chunk, width), lambda i: (i, 0))
    out_types = [jax.ShapeDtypeStruct(users.shape, F32)]
    if low_out:
        out_types.append(jax.ShapeDtypeStruct(users.shape, BF16))
    return pl.pallas_call(
        functools.partial(users_kernel, number, low_out),
        grid=(user_rows // chunk,),
        out_shape=out_types,
        in_specs=[block]
        + [pl.BlockSpec((tile, width), lambda i: (0, 0))] * number
        + [pl.BlockSpec((chunk, tile), lambda i: (i, 0))] * number,
        out_specs=[block] * len(out_types),
        compiler_params=pltpu.CompilerParams(vmem_limit_bytes=12 * MIB),
        cost_estimate=pl.CostEstimate(
            flops=2 * user_rows * tile * number * width, bytes_accessed=4 * MIB, transcendentals=0
        ),
        name="users",
    )(users, *items, *residuals)


def updated_items(items, grad):
    return items + 0.003 * (grad - 0.05 * items)


def paired_shards(user_factors, item_factors, tile_rows, tile_columns, tile_counts, ratings):
    step_total, tile = ratings.shape[2], ratings.shape[-1]
    per_shard = item_factors.shape[0] // tile
    column_tiles = per_shard * lax.axis_size("users")
    halves = range(per_shard)
    parts = [item_factors[h * tile : (h + 1) * tile] for h in halves]
    low = [part.astype(BF16) for part in parts]
    users_now = user_factors
    users_low = user_factors.astype(BF16)
    held = {0: low, 2: [route(block, 0, 2) for block in low]}
    for step in range(step_total):
        dense = dense_ratings(
            step, per_shard, column_tiles, users_now.shape[0], tile_rows, tile_columns, tile_counts, ratings
        )
        for d in (0, 2):
            held[d + 1] = [route(block, 0, 1) for block in held[d]]
        residuals, grads = {}, {}
        for h in halves:
            for d in (2, 3, 0, 1):
                residuals[d, h], grads[d, h] = terms(
                    (d * per_shard + h,), users_low, dense, [held[d][h]]
                )
        sums = []
        for h in halves:
            far = grads[3, h] + route(grads[2, h], 0, 1)
            near = grads[0, h] + route(grads[1, h], 0, 1)
            sums.append(near + route(far, 0, 3))
        parts = [updated_items(part, grad) for part, grad in zip(parts, sums)]
        last = step == step_total - 1
        order = [(d, h) for h in halves for d in range(4)]
        results = update_users(
            users_now, [held[d][h] for d, h in order], [residuals[k] for k in order], not last
        )
        users_now = results[0]
        if not last:
            users_low = results[1]
            low = [part.astype(BF16) for part in parts]
            held = {0: [], 2: []}
            for block in low:
                held[0].append(route(block, 1, 0))
                held[2].append(route(block, 1, 2))
            parts = [route(part, 1, 0) for part in parts]
    return users_now, jnp.concatenate(parts, axis=0)


def gathered_shards(user_factors, item_factors, tile_rows, tile_columns, tile_counts, ratings):
    step_total, tile = ratings.shape[2], ratings.shape[-1]
    users_now, item_part = user_factors, item_factors
    for step in range(step_total):
        block = lax.all_gather(item_part.astype(BF16), "users", axis=0, tiled=True)
        column_tiles = block.shape[0] // tile
        items = [block[j * tile : (j + 1) * tile] for j in range(column_tiles)]
        dense = dense_ratings(
            step, 0, column_tiles, users_now.shape[0], tile_rows, tile_columns, tile_counts, ratings
        )
        users_low = users_now.astype(BF16)
        residuals, grads = [], []
        for j in range(column_tiles):
            residual, grad = terms((j,), users_low, dense, [items[j]])
            residuals.append(residual)
            grads.append(grad)
        grad_part = lax.psum_scatter(
            jnp.concatenate(grads, axis=0), "users", scatter_dimension=0, tiled=True
        )
        users_now = update_users(users_now, items, residuals, False)[0]
        item_part = updated_items(item_part, grad_part)
        if step < step_total - 1:
            item_part = route(item_part, 1, 0)
    return users_now, item_part


def solution(mesh):
    placed = (
        P(("strata", "users"), None),
        P(("strata", "users"), None),
        P("strata", "users", None, None),
        P("strata", "users", None, None),
        P("strata", "users", None),
        P("strata", "users", None, None, None, None),
    )

    def shards(user_factors, item_factors, *lists):
        tile = lists[-1].shape[-1]
        paired = mesh.shape["users"] == 4 and item_factors.shape[0] % tile == 0
        body = paired_shards if paired else gathered_shards
        return body(user_factors, item_factors, *lists)

    return jax.shard_map(
        shards,
        mesh=mesh,
        in_specs=placed,
        out_specs=(P(("strata", "users"), None), P(("strata", "users"), None)),
        check_vma=False,
    )
```

```python
import functools

import jax
import jax.numpy as jnp
from jax import lax
from jax.experimental import pallas as pl
from jax.experimental.pallas import tpu as pltpu
from jax.sharding import PartitionSpec as P

F32 = jnp.float32
BF16 = jnp.bfloat16
VMEM = pl.BlockSpec(memory_space=pltpu.VMEM)
SMEM = pl.BlockSpec(memory_space=pltpu.SMEM)
ANY = pl.BlockSpec(memory_space=pl.ANY)
BOTH_ROWS = (((0,), (0,)), ((), ()))
BOTH_COLUMNS = (((1,), (1,)), ((), ()))
MIB = 1 << 20


def route(block, strata_shift, users_flip):
    strata, users = lax.axis_size("strata"), lax.axis_size("users")
    pairs = [
        (s * users + u, ((s + strata_shift) % strata) * users + (u ^ users_flip))
        for s in range(strata)
        for u in range(users)
    ]
    return lax.ppermute(block, ("strata", "users"), pairs)


def dense_kernel(
    step, tiles_per_shard, group, counts_hbm, rows_hbm, columns_hbm, ratings_hbm, dense_ref,
    tiles, counts_ref, rows_ref, columns_ref, arrived, listed,
):
    flip = lax.axis_index("users") * tiles_per_shard
    lists = [
        pltpu.make_async_copy(counts_hbm, counts_ref, listed.at[0]),
        pltpu.make_async_copy(rows_hbm, rows_ref, listed.at[1]),
        pltpu.make_async_copy(columns_hbm, columns_ref, listed.at[2]),
    ]

    def rating_copy(g):
        some = pl.ds(g * group, group)
        return pltpu.make_async_copy(
            ratings_hbm.at[0, 0, step, some], tiles.at[some], arrived.at[g]
        )

    groups = tiles.shape[0] // group
    for copy in lists:
        copy.start()
    for g in range(groups):
        rating_copy(g).start()

    @pl.loop(0, dense_ref.shape[0])
    def _(j):
        dense_ref[j] = jnp.zeros(dense_ref.shape[1:], BF16)

    for copy in lists:
        copy.wait()
    count = counts_ref[0, 0, step]

    @pl.loop(0, groups)
    def _(g):
        rating_copy(g).wait()

        @pl.when(g * group < count)
        def _():
            for k in range(group):
                m = g * group + k
                j = columns_ref[0, 0, step, m] ^ flip
                r = rows_ref[0, 0, step, m]
                rating = jnp.where(m < count, tiles[m], 0)
                dense_ref[j, r] = rating.astype(F32).astype(BF16).T


def dense_ratings(step, tiles_per_shard, column_tiles, user_rows, tile_rows, tile_columns, tile_counts, ratings):
    slots, tile = ratings.shape[3], ratings.shape[4]
    group = 8 if slots % 8 == 0 else 1
    operands = [
        pltpu.with_memory_space_constraint(x, pltpu.HBM)
        for x in (tile_counts, tile_rows, tile_columns, ratings)
    ]
    return pl.pallas_call(
        functools.partial(dense_kernel, step, tiles_per_shard, group),
        out_shape=jax.ShapeDtypeStruct((column_tiles, user_rows // tile, tile, tile), BF16),
        in_specs=[pl.BlockSpec(memory_space=pltpu.HBM)] * 4,
        out_specs=VMEM,
        scratch_shapes=[
            pltpu.VMEM((slots, tile, tile), jnp.int32),
            pltpu.SMEM(tile_counts.shape, jnp.int32),
            pltpu.SMEM(tile_rows.shape, jnp.int32),
            pltpu.SMEM(tile_columns.shape, jnp.int32),
            pltpu.SemaphoreType.DMA((slots // group,)),
            pltpu.SemaphoreType.DMA((3,)),
        ],
        compiler_params=pltpu.CompilerParams(vmem_limit_bytes=12 * MIB),
        cost_estimate=pl.CostEstimate(flops=2 * 10**9, bytes_accessed=8 * MIB, transcendentals=0),
        name=f"dense_{step}",
    )(*operands)


def terms_kernel(columns, users_ref, dense_ref, *refs):
    number = len(columns)
    item_refs, residual_refs, grad_refs = refs[:number], refs[number : 2 * number], refs[2 * number :]
    tile = item_refs[0].shape[0]
    users = users_ref[...]
    for k, j in enumerate(columns):
        predicted = lax.dot_general(
            item_refs[k][...], users, BOTH_COLUMNS, preferred_element_type=F32
        )
        residuals = []
        for r in range(dense_ref.shape[1]):
            rating = dense_ref[j, r].astype(F32)
            residual = jnp.where(
                rating > 0, rating - predicted[:, r * tile : (r + 1) * tile], 0.0
            ).astype(BF16)
            residual_refs[k][r] = residual
            residuals.append(residual)
        grad_refs[k][...] = jnp.dot(
            jnp.concatenate(residuals, axis=1), users, preferred_element_type=F32
        )


def terms(columns, users_low, dense, items):
    user_rows, width = users_low.shape
    tile = items[0].shape[0]
    number = len(columns)
    return pl.pallas_call(
        functools.partial(terms_kernel, columns),
        out_shape=[jax.ShapeDtypeStruct((user_rows // tile, tile, tile), BF16)] * number
        + [jax.ShapeDtypeStruct((tile, width), F32)] * number,
        in_specs=[VMEM] * (2 + number),
        out_specs=[VMEM] * (2 * number),
        compiler_params=pltpu.CompilerParams(vmem_limit_bytes=16 * MIB),
        cost_estimate=pl.CostEstimate(
            flops=4 * user_rows * tile * width * number, bytes_accessed=MIB, transcendentals=0
        ),
        name="terms_" + "_".join(map(str, columns)),
    )(users_low, dense, *items)


def users_kernel(number, low_out, users_ref, *refs):
    item_refs, residual_refs, outs = refs[:number], refs[number : 2 * number], refs[2 * number :]
    items = jnp.concatenate([ref[...] for ref in item_refs], axis=0)
    tile = item_refs[0].shape[0]
    for r in range(residual_refs[0].shape[0]):
        residual = jnp.concatenate([ref[r] for ref in residual_refs], axis=0)
        total = lax.dot_general(residual, items, BOTH_ROWS, preferred_element_type=F32)
        rows = slice(r * tile, (r + 1) * tile)
        users = users_ref[rows, :]
        updated = users + 0.01 * (total - 0.05 * users)
        outs[0][rows, :] = updated
        if low_out:
            outs[1][rows, :] = updated.astype(BF16)


def update_users(users, items, residuals, low_out):
    user_rows, width = users.shape
    number = len(items)
    tile = items[0].shape[0]
    group = 2
    block = pl.BlockSpec((group * tile, width), lambda i: (i, 0))
    out_types = [jax.ShapeDtypeStruct(users.shape, F32)]
    if low_out:
        out_types.append(jax.ShapeDtypeStruct(users.shape, BF16))
    return pl.pallas_call(
        functools.partial(users_kernel, number, low_out),
        grid=(user_rows // (group * tile),),
        out_shape=out_types,
        in_specs=[block]
        + [pl.BlockSpec((tile, width), lambda i: (0, 0))] * number
        + [pl.BlockSpec((group, tile, tile), lambda i: (i, 0, 0))] * number,
        out_specs=[block] * len(out_types),
        compiler_params=pltpu.CompilerParams(vmem_limit_bytes=12 * MIB),
        cost_estimate=pl.CostEstimate(
            flops=2 * user_rows * tile * number * width, bytes_accessed=4 * MIB, transcendentals=0
        ),
        name="users",
    )(users, *items, *residuals)


def updated_items(items, grad):
    return items + 0.003 * (grad - 0.05 * items)


def paired_shards(user_factors, item_factors, tile_rows, tile_columns, tile_counts, ratings):
    step_total, tile = ratings.shape[2], ratings.shape[-1]
    per_shard = item_factors.shape[0] // tile
    column_tiles = per_shard * lax.axis_size("users")
    halves = range(per_shard)
    parts = [item_factors[h * tile : (h + 1) * tile] for h in halves]
    low = [part.astype(BF16) for part in parts]
    users_now = user_factors
    users_low = user_factors.astype(BF16)
    held = {0: low, 2: [route(block, 0, 2) for block in low]}
    for step in range(step_total):
        dense = dense_ratings(
            step, per_shard, column_tiles, users_now.shape[0], tile_rows, tile_columns, tile_counts, ratings
        )
        for d in (0, 2):
            held[d + 1] = [route(block, 0, 1) for block in held[d]]
        residuals, grads = {}, {}
        for h in halves:
            for d in (2, 3, 0, 1):
                residuals[d, h], grads[d, h] = terms(
                    (d * per_shard + h,), users_low, dense, [held[d][h]]
                )
        sums = []
        for h in halves:
            far = grads[3, h] + route(grads[2, h], 0, 1)
            near = grads[0, h] + route(grads[1, h], 0, 1)
            sums.append(near + route(far, 0, 3))
        parts = [updated_items(part, grad) for part, grad in zip(parts, sums)]
        last = step == step_total - 1
        order = [(d, h) for h in halves for d in range(4)]
        results = update_users(
            users_now, [held[d][h] for d, h in order], [residuals[k] for k in order], not last
        )
        users_now = results[0]
        if not last:
            users_low = results[1]
            low = [part.astype(BF16) for part in parts]
            held = {0: [], 2: []}
            for block in low:
                held[0].append(route(block, 1, 0))
                held[2].append(route(block, 1, 2))
            parts = [route(part, 1, 0) for part in parts]
    return users_now, jnp.concatenate(parts, axis=0)


def gathered_shards(user_factors, item_factors, tile_rows, tile_columns, tile_counts, ratings):
    step_total, tile = ratings.shape[2], ratings.shape[-1]
    users_now, item_part = user_factors, item_factors
    for step in range(step_total):
        block = lax.all_gather(item_part.astype(BF16), "users", axis=0, tiled=True)
        column_tiles = block.shape[0] // tile
        items = [block[j * tile : (j + 1) * tile] for j in range(column_tiles)]
        dense = dense_ratings(
            step, 0, column_tiles, users_now.shape[0], tile_rows, tile_columns, tile_counts, ratings
        )
        users_low = users_now.astype(BF16)
        residuals, grads = [], []
        for j in range(column_tiles):
            residual, grad = terms((j,), users_low, dense, [items[j]])
            residuals.append(residual)
            grads.append(grad)
        grad_part = lax.psum_scatter(
            jnp.concatenate(grads, axis=0), "users", scatter_dimension=0, tiled=True
        )
        users_now = update_users(users_now, items, residuals, False)[0]
        item_part = updated_items(item_part, grad_part)
        if step < step_total - 1:
            item_part = route(item_part, 1, 0)
    return users_now, item_part


def solution(mesh):
    placed = (
        P(("strata", "users"), None),
        P(("strata", "users"), None),
        P("strata", "users", None, None),
        P("strata", "users", None, None),
        P("strata", "users", None),
        P("strata", "users", None, None, None, None),
    )

    def shards(user_factors, item_factors, *lists):
        tile = lists[-1].shape[-1]
        paired = mesh.shape["users"] == 4 and item_factors.shape[0] % tile == 0
        body = paired_shards if paired else gathered_shards
        return body(user_factors, item_factors, *lists)

    return jax.shard_map(
        shards,
        mesh=mesh,
        in_specs=placed,
        out_specs=(P(("strata", "users"), None), P(("strata", "users"), None)),
        check_vma=False,
    )
```

```python
import functools

import jax
import jax.numpy as jnp
from jax import lax
from jax.experimental import pallas as pl
from jax.experimental.pallas import tpu as pltpu
from jax.sharding import PartitionSpec as P


F32 = jnp.float32
BF16 = jnp.bfloat16
VMEM = pl.BlockSpec(memory_space=pltpu.VMEM)
SMEM = pl.BlockSpec(memory_space=pltpu.SMEM)
ANY = pl.BlockSpec(memory_space=pl.ANY)
BOTH_ROWS = (((0,), (0,)), ((), ()))
BOTH_COLUMNS = (((1,), (1,)), ((), ()))
MIB = 1 << 20


def route(block, strata_shift, users_flip):
    strata, users = lax.axis_size("strata"), lax.axis_size("users")
    pairs = [
        (s * users + u, ((s + strata_shift) % strata) * users + (u ^ users_flip))
        for s in range(strata)
        for u in range(users)
    ]
    return lax.ppermute(block, ("strata", "users"), pairs)


def dense_kernel(
    step, tiles_per_shard, group, counts_hbm, rows_hbm, columns_hbm, ratings_hbm, dense_ref,
    tiles, counts_ref, rows_ref, columns_ref, arrived, listed,
):
    flip = lax.axis_index("users") * tiles_per_shard
    lists = [
        pltpu.make_async_copy(counts_hbm, counts_ref, listed.at[0]),
        pltpu.make_async_copy(rows_hbm, rows_ref, listed.at[1]),
        pltpu.make_async_copy(columns_hbm, columns_ref, listed.at[2]),
    ]

    def rating_copy(g):
        some = pl.ds(g * group, group)
        return pltpu.make_async_copy(
            ratings_hbm.at[0, 0, step, some], tiles.at[some], arrived.at[g]
        )

    groups = tiles.shape[0] // group
    for copy in lists:
        copy.start()
    for g in range(groups):
        rating_copy(g).start()

    @pl.loop(0, dense_ref.shape[0])
    def _(j):
        dense_ref[j] = jnp.zeros(dense_ref.shape[1:], BF16)

    for copy in lists:
        copy.wait()
    count = counts_ref[0, 0, step]

    @pl.loop(0, groups)
    def _(g):
        rating_copy(g).wait()

        @pl.when(g * group < count)
        def _():
            for k in range(group):
                m = g * group + k
                j = columns_ref[0, 0, step, m] ^ flip
                r = rows_ref[0, 0, step, m]
                rating = jnp.where(m < count, tiles[m], 0)
                dense_ref[j, r] = rating.astype(F32).astype(BF16).T


def dense_ratings(step, tiles_per_shard, column_tiles, user_rows, tile_rows, tile_columns, tile_counts, ratings):
    slots, tile = ratings.shape[3], ratings.shape[4]
    group = 8 if slots % 8 == 0 else 1
    operands = [
        pltpu.with_memory_space_constraint(x, pltpu.HBM)
        for x in (tile_counts, tile_rows, tile_columns, ratings)
    ]
    return pl.pallas_call(
        functools.partial(dense_kernel, step, tiles_per_shard, group),
        out_shape=jax.ShapeDtypeStruct((column_tiles, user_rows // tile, tile, tile), BF16),
        in_specs=[pl.BlockSpec(memory_space=pltpu.HBM)] * 4,
        out_specs=VMEM,
        scratch_shapes=[
            pltpu.VMEM((slots, tile, tile), jnp.int32),
            pltpu.SMEM(tile_counts.shape, jnp.int32),
            pltpu.SMEM(tile_rows.shape, jnp.int32),
            pltpu.SMEM(tile_columns.shape, jnp.int32),
            pltpu.SemaphoreType.DMA((slots // group,)),
            pltpu.SemaphoreType.DMA((3,)),
        ],
        compiler_params=pltpu.CompilerParams(vmem_limit_bytes=12 * MIB),
        cost_estimate=pl.CostEstimate(flops=2 * 10**9, bytes_accessed=8 * MIB, transcendentals=0),
    )(*operands)


def terms_kernel(columns, sizes, chunk, users_ref, dense_ref, *refs):
    item_refs, (residual_ref, *grad_refs) = refs[: len(refs) - 1 - len(sizes)], refs[-1 - len(sizes) :]
    tile = dense_ref.shape[-1]
    per_chunk = chunk // tile
    items = jnp.concatenate([ref[...] for ref in item_refs], axis=0)
    chunks = users_ref.shape[0] // chunk

    def users(i):
        return users_ref[i * chunk : (i + 1) * chunk, :]

    def predict(i):
        return lax.dot_general(items, users(i), BOTH_COLUMNS, preferred_element_type=F32)

    grad = None
    ahead = predict(0)
    for i in range(chunks):
        predicted = ahead
        if i + 1 < chunks:
            ahead = predict(i + 1)
        residuals = []
        for q in range(per_chunk):
            r = i * per_chunk + q
            rating = jnp.concatenate([dense_ref[j, r] for j in columns], axis=0).astype(F32)
            residual = jnp.where(
                rating > 0, rating - predicted[:, q * tile : (q + 1) * tile], 0.0
            ).astype(BF16)
            residual_ref[r] = residual
            residuals.append(residual)
        part = jnp.dot(jnp.concatenate(residuals, axis=1), users(i), preferred_element_type=F32)
        grad = part if grad is None else grad + part
    start = 0
    for ref in grad_refs:
        ref[...] = grad[start : start + ref.shape[0]]
        start += ref.shape[0]


def terms(columns, sizes, users_low, dense, items):
    user_rows, width = users_low.shape
    tile = dense.shape[-1]
    rows = tile * len(columns)
    return pl.pallas_call(
        functools.partial(terms_kernel, columns, sizes, min(4 * tile, user_rows)),
        out_shape=[jax.ShapeDtypeStruct((user_rows // tile, rows, tile), BF16)]
        + [jax.ShapeDtypeStruct((size, width), F32) for size in sizes],
        in_specs=[VMEM] * (2 + len(items)),
        out_specs=[VMEM] * (1 + len(sizes)),
        compiler_params=pltpu.CompilerParams(vmem_limit_bytes=16 * MIB),
        cost_estimate=pl.CostEstimate(
            flops=4 * user_rows * rows * width, bytes_accessed=MIB, transcendentals=0
        ),
    )(users_low, dense, *items)


def users_kernel(number, chunk, low_out, users_ref, *refs):
    item_refs, refs = refs[:number], refs[number:]
    items = jnp.concatenate([ref[...] for ref in item_refs], axis=0)
    tile = refs[0].shape[-1]
    if low_out:
        *residual_refs, out_ref, low_ref = refs
    else:
        *residual_refs, out_hbm, out_ref, sent = refs
    copies = []
    for i in range(users_ref.shape[0] // chunk):
        rows = slice(i * chunk, (i + 1) * chunk)
        residual = jnp.concatenate(
            [
                jnp.concatenate([ref[r] for ref in residual_refs], axis=0)
                for r in range(i * chunk // tile, (i + 1) * chunk // tile)
            ],
            axis=1,
        )
        total = lax.dot_general(residual, items, BOTH_ROWS, preferred_element_type=F32)
        users = users_ref[rows, :]
        updated = users + 0.01 * (total - 0.05 * users)
        out_ref[rows, :] = updated
        if low_out:
            low_ref[rows, :] = updated.astype(BF16)
        else:
            copies.append(pltpu.make_async_copy(out_ref.at[rows], out_hbm.at[rows], sent.at[i]))
            copies[-1].start()
    for copy in copies:
        copy.wait()


def update_users(users, items, residuals, low_out):
    user_rows, width = users.shape
    tile = residuals[0].shape[-1]
    chunk = min(2 * tile, user_rows)
    item_rows = sum(block.shape[0] for block in items)
    full = jax.ShapeDtypeStruct(users.shape, F32)
    if low_out:
        out_shape, out_specs, scratch = [full, jax.ShapeDtypeStruct(users.shape, BF16)], [VMEM] * 2, []
    else:
        out_shape, out_specs = [full], [pl.BlockSpec(memory_space=pltpu.HBM)]
        scratch = [pltpu.VMEM(users.shape, F32), pltpu.SemaphoreType.DMA((user_rows // chunk,))]
    return pl.pallas_call(
        functools.partial(users_kernel, len(items), chunk, low_out),
        out_shape=out_shape,
        in_specs=[VMEM] * (1 + len(items) + len(residuals)),
        out_specs=out_specs,
        scratch_shapes=scratch,
        compiler_params=pltpu.CompilerParams(vmem_limit_bytes=12 * MIB),
        cost_estimate=pl.CostEstimate(
            flops=2 * user_rows * item_rows * width, bytes_accessed=4 * MIB, transcendentals=0
        ),
        name="users",
    )(users, *items, *residuals)


def updated_items(items, grad):
    return items + 0.003 * (grad - 0.05 * items)


def after(value, *earlier):
    return lax.optimization_barrier((value, *earlier))[0]


def paired_shards(user_factors, item_factors, tile_rows, tile_columns, tile_counts, ratings):
    step_total, tile = ratings.shape[2], ratings.shape[-1]
    per_shard = item_factors.shape[0] // tile
    column_tiles = per_shard * lax.axis_size("users")
    halves = range(per_shard)
    low = item_factors.astype(BF16)
    users_now, items_now = user_factors, item_factors
    held = {0: [low], 1: [route(low, 0, 1)], 2: [route(low, 0, 2)]}
    mark = []

    def ratings_of(step):
        return dense_ratings(
            step, per_shard, column_tiles, user_factors.shape[0],
            after(tile_rows, *mark), tile_columns, tile_counts, ratings,
        )

    dense = ratings_of(0)
    users_low = after(user_factors, dense).astype(BF16)
    for step in range(step_total):
        pieces = len(held[2])
        items_in, residuals, sums = [], [], []

        def run(*which):
            items = [held[d][p] for d, p in which]
            sizes = tuple(block.shape[0] for block in items)
            columns = tuple(
                d * per_shard + p * size // tile + k
                for (d, p), size in zip(which, sizes)
                for k in range(size // tile)
            )
            items[0] = after(items[0], *mark)
            residual, *grads = terms(columns, sizes, users_low, dense, items)
            mark[:] = grads[-1:]
            items_in.extend(held[d][p] for d, p in which)
            residuals.append(residual)
            return grads

        def near():
            own, passed = run((0, 0), (1, 0))
            return own + route(passed, 0, 1)

        def far(p):
            (passed,) = run((2, p))
            passed = route(passed, 0, 1)
            (own,) = run((3, p))
            for k in range(per_shard // pieces):
                rows = slice(k * tile, (k + 1) * tile)
                sums.append(route(own[rows] + passed[rows], 0, 3))

        def update(low_out):
            blocks = list(items_in)
            blocks[0] = after(blocks[0], *mark)
            results = update_users(users_now, blocks, residuals, low_out)
            mark[:] = results[-1:]
            return results

        last = step == step_total - 1
        held[3] = []
        if step == 0:
            near_sum = near()
        for p in range(pieces):
            block = after(held[2][p], *mark) if p else held[2][p]
            held[3].append(route(block, 0, 1))
            far(p)
        if step > 0:
            held[0] = [after(held[0][0], *mark)]
            held[1] = [route(held[0][0], 0, 1)]
            near_sum = near()
        if not last:
            dense = ratings_of(step + 1)
        low_parts, held = [], {2: []}
        users_now, *rest = update(not last)
        parts = []
        for h in halves:
            rows = slice(h * tile, (h + 1) * tile)
            base = updated_items(items_now[rows], after(near_sum, *parts)[rows])
            base = lax.optimization_barrier(base)
            parts.append(base + 0.003 * sums[h])
            if not last:
                low_parts.append(parts[h].astype(BF16))
                held[2].append(route(low_parts[h], 1, 2))
        items_now = jnp.concatenate(parts, axis=0)
        if not last:
            users_low = rest[0]
            held[0] = [route(jnp.concatenate(low_parts, axis=0), 1, 0)]
            items_now = route(after(items_now, *mark), 1, 0)
    return users_now, items_now


def gathered_shards(user_factors, item_factors, tile_rows, tile_columns, tile_counts, ratings):
    step_total, tile = ratings.shape[2], ratings.shape[-1]
    users_now, item_part = user_factors, item_factors
    for step in range(step_total):
        block = lax.all_gather(item_part.astype(BF16), "users", axis=0, tiled=True)
        column_tiles = block.shape[0] // tile
        dense = dense_ratings(
            step, 0, column_tiles, users_now.shape[0], tile_rows, tile_columns, tile_counts, ratings
        )
        residual, grad = terms(
            tuple(range(column_tiles)), block.shape[:1], users_now.astype(BF16), dense, [block]
        )
        grad_part = lax.psum_scatter(grad, "users", scatter_dimension=0, tiled=True)
        users_now = update_users(users_now, [block], [residual], False)[0]
        item_part = updated_items(item_part, grad_part)
        if step < step_total - 1:
            item_part = route(item_part, 1, 0)
    return users_now, item_part


def solution(mesh):
    placed = (
        P(("strata", "users"), None),
        P(("strata", "users"), None),
        P("strata", "users", None, None),
        P("strata", "users", None, None),
        P("strata", "users", None),
        P("strata", "users", None, None, None, None),
    )

    def shards(user_factors, item_factors, *lists):
        tile = lists[-1].shape[-1]
        paired = mesh.shape["users"] == 4 and item_factors.shape[0] % tile == 0
        body = paired_shards if paired else gathered_shards
        return body(user_factors, item_factors, *lists)

    return jax.shard_map(
        shards,
        mesh=mesh,
        in_specs=placed,
        out_specs=(P(("strata", "users"), None), P(("strata", "users"), None)),
        check_vma=False,
    )
```

```python
import functools

import jax
import jax.numpy as jnp
from jax import lax
from jax.experimental import pallas as pl
from jax.experimental.pallas import tpu as pltpu
from jax.sharding import PartitionSpec as P


F32 = jnp.float32
BF16 = jnp.bfloat16
VMEM = pl.BlockSpec(memory_space=pltpu.VMEM)
HBM = pl.BlockSpec(memory_space=pltpu.HBM)
BOTH_ROWS = (((0,), (0,)), ((), ()))
MIB = 1 << 20
CHUNK_TILES = 4
LATENCY_SCALE = 3


def route(block, strata_shift, users_flip):
    strata, users = lax.axis_size("strata"), lax.axis_size("users")
    pairs = [
        (s * users + u, ((s + strata_shift) % strata) * users + (u ^ users_flip))
        for s in range(strata)
        for u in range(users)
    ]
    return lax.ppermute(block, ("strata", "users"), pairs)


def lower_users(users, rows, low_ref, low_t_ref):
    low = users.astype(BF16)
    low_ref[rows, :] = low
    low_t_ref[:, rows] = low.T


def low_shapes(users):
    return [jax.ShapeDtypeStruct(users.shape, BF16), jax.ShapeDtypeStruct(users.shape[::-1], BF16)]


def lower_kernel(chunk, users_ref, low_ref, low_t_ref):
    for i in range(users_ref.shape[0] // chunk):
        rows = slice(i * chunk, (i + 1) * chunk)
        lower_users(users_ref[rows, :], rows, low_ref, low_t_ref)


def lower(users, tile):
    return pl.pallas_call(
        functools.partial(lower_kernel, tile),
        out_shape=low_shapes(users),
        in_specs=[VMEM],
        out_specs=[VMEM] * 2,
        compiler_params=pltpu.CompilerParams(vmem_limit_bytes=8 * MIB),
        cost_estimate=pl.CostEstimate(flops=10**8, bytes_accessed=MIB, transcendentals=0),
        name="lower",
    )(users)


def rating_copies(ratings_hbm, step, tiles, arrived):
    group = tiles.shape[0] // arrived.shape[0]
    return [
        pltpu.make_async_copy(
            ratings_hbm.at[0, 0, step, pl.ds(g * group, group)],
            tiles.at[pl.ds(g * group, group)],
            arrived.at[g],
        )
        for g in range(arrived.shape[0])
    ]


def dense_kernel(step, tiles_per_shard, group, fetched, counts_hbm, rows_hbm, columns_hbm, ratings, dense_ref, *scratch):
    *lists, listed = scratch if fetched else scratch[2:]
    tiles = ratings.at[0, 0, step] if fetched else scratch[0]
    counts_ref, rows_ref, columns_ref = lists
    flip = lax.axis_index("users") * tiles_per_shard
    copies = [
        pltpu.make_async_copy(source, target, listed.at[k])
        for k, (source, target) in enumerate(zip((counts_hbm, rows_hbm, columns_hbm), lists))
    ]
    for copy in copies:
        copy.start()
    if not fetched:
        for copy in rating_copies(ratings, step, tiles, scratch[1]):
            copy.start()

    @pl.loop(0, dense_ref.shape[0])
    def _(j):
        dense_ref[j] = jnp.zeros(dense_ref.shape[1:], BF16)

    for copy in copies:
        copy.wait()
    count = counts_ref[0, 0, step]

    def place(g):
        @pl.when(g * group < count)
        def _():
            for k in range(group):
                m = g * group + k
                j = columns_ref[0, 0, step, m] ^ flip
                r = rows_ref[0, 0, step, m]
                rating = jnp.where(m < count, tiles[m], 0)
                dense_ref[j, r] = rating.astype(F32).astype(BF16).T

    @pl.loop(0, tiles.shape[0] // group)
    def _(g):
        if not fetched:
            some = pl.ds(g * group, group)
            pltpu.make_async_copy(ratings.at[0, 0, step, some], tiles.at[some], scratch[1].at[g]).wait()
        place(g)


def slot_group(slots):
    return 8 if slots % 8 == 0 else 1


def in_hbm(*arrays):
    return [pltpu.with_memory_space_constraint(array, pltpu.HBM) for array in arrays]


def dense_ratings(
    step, tiles_per_shard, column_tiles, user_rows, tile_rows, tile_columns, tile_counts, ratings, fetched=False
):
    slots, tile = ratings.shape[3], ratings.shape[4]
    group = slot_group(slots)
    lists = (tile_counts, tile_rows, tile_columns)
    scratch = [pltpu.SMEM(some.shape, jnp.int32) for some in lists] + [pltpu.SemaphoreType.DMA((3,))]
    if not fetched:
        scratch = [
            pltpu.VMEM((slots, tile, tile), jnp.int32), pltpu.SemaphoreType.DMA((slots // group,)), *scratch
        ]
        operands, last_spec = in_hbm(*lists, ratings), HBM
    else:
        operands, last_spec = [*in_hbm(*lists), ratings], VMEM
    return pl.pallas_call(
        functools.partial(dense_kernel, step, tiles_per_shard, group, fetched),
        out_shape=jax.ShapeDtypeStruct((column_tiles, user_rows // tile, tile, tile), BF16),
        in_specs=[HBM] * 3 + [last_spec],
        out_specs=VMEM,
        scratch_shapes=scratch,
        compiler_params=pltpu.CompilerParams(vmem_limit_bytes=12 * MIB),
        cost_estimate=pl.CostEstimate(flops=2 * 10**9, bytes_accessed=8 * MIB, transcendentals=0),
    )(*operands)


def terms_kernel(columns, sizes, chunk, users_ref, users_t_ref, dense_ref, *refs):
    item_refs, (residual_ref, *grad_refs) = refs[: len(refs) - 1 - len(sizes)], refs[-1 - len(sizes) :]
    tile = dense_ref.shape[-1]
    per_chunk = chunk // tile
    items = jnp.concatenate([ref[...] for ref in item_refs], axis=0)
    chunks = users_ref.shape[0] // chunk

    def users(i):
        return users_ref[i * chunk : (i + 1) * chunk, :]

    def predict(i):
        users_t = users_t_ref[:, i * chunk : (i + 1) * chunk]
        return jnp.dot(items, users_t, preferred_element_type=F32)

    grad = None
    ahead = predict(0)
    for i in range(chunks):
        predicted = ahead
        if i + 1 < chunks:
            ahead = predict(i + 1)
        residuals = []
        for q in range(per_chunk):
            r = i * per_chunk + q
            rating = jnp.concatenate([dense_ref[j, r] for j in columns], axis=0).astype(F32)
            residual = jnp.where(
                rating > 0, rating - predicted[:, q * tile : (q + 1) * tile], 0.0
            ).astype(BF16)
            residual_ref[r] = residual
            residuals.append(residual)
        part = jnp.dot(jnp.concatenate(residuals, axis=1), users(i), preferred_element_type=F32)
        grad = part if grad is None else grad + part
    start = 0
    for ref in grad_refs:
        ref[...] = grad[start : start + ref.shape[0]]
        start += ref.shape[0]


def terms(columns, sizes, lowered, dense, items):
    user_rows, width = lowered[0].shape
    tile = dense.shape[-1]
    rows = tile * len(columns)
    return pl.pallas_call(
        functools.partial(terms_kernel, columns, sizes, min(CHUNK_TILES * tile, user_rows)),
        out_shape=[jax.ShapeDtypeStruct((user_rows // tile, rows, tile), BF16)]
        + [jax.ShapeDtypeStruct((size, width), F32) for size in sizes],
        in_specs=[VMEM] * (3 + len(items)),
        out_specs=[VMEM] * (1 + len(sizes)),
        compiler_params=pltpu.CompilerParams(vmem_limit_bytes=16 * MIB),
        cost_estimate=pl.CostEstimate(
            flops=LATENCY_SCALE * 4 * user_rows * rows * width, bytes_accessed=MIB, transcendentals=0
        ),
    )(*lowered, dense, *items)


def users_kernel(number, chunk, last, users_ref, *refs):
    item_refs, refs = refs[:number], refs[number:]
    items = jnp.concatenate([ref[...] for ref in item_refs], axis=0)
    tile = refs[0].shape[-1]
    copies = []
    if last:
        *residual_refs, out_hbm, out_ref, sent = refs
    else:
        *residual_refs, out_ref, low_ref, low_t_ref = refs
    for i in range(users_ref.shape[0] // chunk):
        rows = slice(i * chunk, (i + 1) * chunk)
        residual = jnp.concatenate(
            [
                jnp.concatenate([ref[r] for ref in residual_refs], axis=0)
                for r in range(i * chunk // tile, (i + 1) * chunk // tile)
            ],
            axis=1,
        )
        total = lax.dot_general(residual, items, BOTH_ROWS, preferred_element_type=F32)
        users = users_ref[rows, :]
        updated = users + 0.01 * (total - 0.05 * users)
        out_ref[rows, :] = updated
        if last:
            copies.append(pltpu.make_async_copy(out_ref.at[rows], out_hbm.at[rows], sent.at[i]))
            copies[-1].start()
        else:
            lower_users(updated, rows, low_ref, low_t_ref)
    for copy in copies:
        copy.wait()


def update_users(users, items, residuals, last):
    user_rows, width = users.shape
    tile = residuals[0].shape[-1]
    chunk = min(2 * tile, user_rows)
    item_rows = sum(block.shape[0] for block in items)
    full = jax.ShapeDtypeStruct(users.shape, F32)
    if last:
        out_shape, out_specs = [full], [HBM]
        scratch = [pltpu.VMEM(users.shape, F32), pltpu.SemaphoreType.DMA((user_rows // chunk,))]
    else:
        out_shape, out_specs, scratch = [full, *low_shapes(users)], [VMEM] * 3, []
    return pl.pallas_call(
        functools.partial(users_kernel, len(items), chunk, last),
        out_shape=out_shape,
        in_specs=[VMEM] * (1 + len(items) + len(residuals)),
        out_specs=out_specs,
        scratch_shapes=scratch,
        compiler_params=pltpu.CompilerParams(vmem_limit_bytes=12 * MIB),
        cost_estimate=pl.CostEstimate(
            flops=LATENCY_SCALE * 2 * user_rows * item_rows * width, bytes_accessed=4 * MIB, transcendentals=0
        ),
        name="users",
    )(users, *items, *residuals)


def updated_items(items, grad):
    return items + 0.003 * (grad - 0.05 * items)


def after(value, *earlier):
    return lax.optimization_barrier((value, *earlier))[0]


def paired_shards(user_factors, item_factors, tile_rows, tile_columns, tile_counts, ratings):
    step_total, tile = ratings.shape[2], ratings.shape[-1]
    per_shard = item_factors.shape[0] // tile
    column_tiles = per_shard * lax.axis_size("users")
    parts_rows = [slice(h * tile, (h + 1) * tile) for h in range(per_shard)]
    low = item_factors.astype(BF16)
    users_now, items_now = user_factors, item_factors
    held = {0: [low], 1: [route(low, 0, 1)], 2: [route(low, 0, 2)]}
    mark = []

    def ratings_of(step):
        dense = dense_ratings(
            step, per_shard, column_tiles, user_factors.shape[0],
            after(tile_rows, *mark), tile_columns, tile_counts, ratings, step > 0,
        )
        mark[:] = [dense]
        return dense

    dense = ratings_of(0)
    lowered = lower(after(user_factors, dense), tile)
    mark[:] = lowered[:1]
    for step in range(step_total):
        last = step == step_total - 1
        items_in, residuals, sums = [], [], []

        def run(d, block, first=0):
            blocks = block if isinstance(block, list) else [block]
            sizes = tuple(some.shape[0] for some in blocks)
            columns = tuple(
                (d + i) * per_shard + first + k for i, size in enumerate(sizes) for k in range(size // tile)
            )
            residual, *grads = terms(
                columns, sizes, lowered, dense, [after(blocks[0], *mark), *blocks[1:]]
            )
            mark[:] = grads[-1:]
            items_in.extend(blocks)
            residuals.append(residual)
            return grads

        def near():
            own, passed = run(0, [held[0][0], held[1][0]])
            return own + route(passed, 0, 1)

        if step == 0:
            near_sum = near()
        for p, block in enumerate(held[2]):
            first = p * block.shape[0] // tile
            shared = route(after(block, *mark), 0, 1)
            (passed,) = run(2, block, first)
            passed = route(passed, 0, 1)
            if step > 0 and p == len(held[2]) - 1:
                held[1] = [route(after(held[0][0], *mark), 0, 1)]
            for k in range(block.shape[0] // tile):
                h, rows = first + k, parts_rows[k]
                (own,) = run(3, shared[rows], h)
                own = lax.optimization_barrier(own + passed[rows])
                mark.append(own)
                sums.append(route(own, 0, 3))
        if step > 0:
            near_sum = near()
        blocks = list(items_in)
        blocks[0] = after(blocks[0], *mark)
        users_now, *lowered = update_users(users_now, blocks, residuals, last)
        if last:
            return users_now, updated_items(items_now, near_sum + jnp.concatenate(sums, axis=0))
        mark[:] = lowered[:1]
        dense = ratings_of(step + 1)
        parts, low_parts = [], []
        for h, rows in enumerate(parts_rows):
            base = updated_items(items_now[rows], after(near_sum, *parts)[rows])
            parts.append(lax.optimization_barrier(base) + 0.003 * sums[h])
            low_parts.append(parts[h].astype(BF16))
        held = {2: [route(low, 1, 2) for low in low_parts]}
        held[0] = [route(jnp.concatenate(low_parts, axis=0), 1, 0)]
        items_now = after(jnp.concatenate(parts, axis=0), *mark)
        items_now = route(items_now, 1, 0)


def gathered_shards(user_factors, item_factors, tile_rows, tile_columns, tile_counts, ratings):
    step_total, tile = ratings.shape[2], ratings.shape[-1]
    users_now, item_part = user_factors, item_factors
    for step in range(step_total):
        block = lax.all_gather(item_part.astype(BF16), "users", axis=0, tiled=True)
        column_tiles = block.shape[0] // tile
        dense = dense_ratings(
            step, 0, column_tiles, users_now.shape[0], tile_rows, tile_columns, tile_counts, ratings
        )
        lowered = lower(users_now, tile)
        residual, grad = terms(tuple(range(column_tiles)), block.shape[:1], lowered, dense, [block])
        grad_part = lax.psum_scatter(grad, "users", scatter_dimension=0, tiled=True)
        users_now = update_users(users_now, [block], [residual], True)[0]
        item_part = updated_items(item_part, grad_part)
        if step < step_total - 1:
            item_part = route(item_part, 1, 0)
    return users_now, item_part


def solution(mesh):
    placed = (
        P(("strata", "users"), None),
        P(("strata", "users"), None),
        P("strata", "users", None, None),
        P("strata", "users", None, None),
        P("strata", "users", None),
        P("strata", "users", None, None, None, None),
    )

    def shards(user_factors, item_factors, *lists):
        tile = lists[-1].shape[-1]
        paired = mesh.shape["users"] == 4 and item_factors.shape[0] % tile == 0
        body = paired_shards if paired else gathered_shards
        return body(user_factors, item_factors, *lists)

    return jax.shard_map(
        shards,
        mesh=mesh,
        in_specs=placed,
        out_specs=(P(("strata", "users"), None), P(("strata", "users"), None)),
        check_vma=False,
    )
```

```python
import functools

import jax
import jax.numpy as jnp
from jax import lax
from jax.experimental import pallas as pl
from jax.experimental.pallas import tpu as pltpu
from jax.sharding import PartitionSpec as P


F32 = jnp.float32
BF16 = jnp.bfloat16
VMEM = pl.BlockSpec(memory_space=pltpu.VMEM)
HBM = pl.BlockSpec(memory_space=pltpu.HBM)
BOTH_ROWS = (((0,), (0,)), ((), ()))
MIB = 1 << 20
CHUNK_TILES = 2
LOOKAHEAD = 2
LATENCY_SCALES = (1, 3)


def route(block, strata_shift, users_flip):
    strata, users = lax.axis_size("strata"), lax.axis_size("users")
    pairs = [
        (s * users + u, ((s + strata_shift) % strata) * users + (u ^ users_flip))
        for s in range(strata)
        for u in range(users)
    ]
    return lax.ppermute(block, ("strata", "users"), pairs)


def lower_users(users, rows, low_ref, low_t_ref):
    low = users.astype(BF16)
    low_ref[rows, :] = low
    low_t_ref[:, rows] = low.T


def low_shapes(users):
    return [jax.ShapeDtypeStruct(users.shape, BF16), jax.ShapeDtypeStruct(users.shape[::-1], BF16)]


def lower_kernel(chunk, users_ref, low_ref, low_t_ref):
    for i in range(users_ref.shape[0] // chunk):
        rows = slice(i * chunk, (i + 1) * chunk)
        lower_users(users_ref[rows, :], rows, low_ref, low_t_ref)


def lower(users, tile):
    return pl.pallas_call(
        functools.partial(lower_kernel, tile),
        out_shape=low_shapes(users),
        in_specs=[VMEM],
        out_specs=[VMEM] * 2,
        compiler_params=pltpu.CompilerParams(vmem_limit_bytes=8 * MIB),
        cost_estimate=pl.CostEstimate(flops=10**8, bytes_accessed=MIB, transcendentals=0),
        name="lower",
    )(users)


def rating_copies(ratings_hbm, step, tiles, arrived):
    group = tiles.shape[0] // arrived.shape[0]
    return [
        pltpu.make_async_copy(
            ratings_hbm.at[0, 0, step, pl.ds(g * group, group)],
            tiles.at[pl.ds(g * group, group)],
            arrived.at[g],
        )
        for g in range(arrived.shape[0])
    ]


def dense_kernel(step, tiles_per_shard, group, fetched, counts_hbm, rows_hbm, columns_hbm, ratings, dense_ref, *scratch):
    *lists, listed = scratch if fetched else scratch[2:]
    tiles = ratings.at[0, 0, step] if fetched else scratch[0]
    counts_ref, rows_ref, columns_ref = lists
    flip = lax.axis_index("users") * tiles_per_shard
    copies = [
        pltpu.make_async_copy(source, target, listed.at[k])
        for k, (source, target) in enumerate(zip((counts_hbm, rows_hbm, columns_hbm), lists))
    ]
    for copy in copies:
        copy.start()
    if not fetched:
        for copy in rating_copies(ratings, step, tiles, scratch[1]):
            copy.start()

    @pl.loop(0, dense_ref.shape[0])
    def _(j):
        dense_ref[j] = jnp.zeros(dense_ref.shape[1:], BF16)

    for copy in copies:
        copy.wait()
    count = counts_ref[0, 0, step]

    def place(g):
        @pl.when(g * group < count)
        def _():
            for k in range(group):
                m = g * group + k
                j = columns_ref[0, 0, step, m] ^ flip
                r = rows_ref[0, 0, step, m]
                rating = jnp.where(m < count, tiles[m], 0)
                dense_ref[j, r] = rating.astype(F32).astype(BF16).T

    @pl.loop(0, tiles.shape[0] // group)
    def _(g):
        if not fetched:
            some = pl.ds(g * group, group)
            pltpu.make_async_copy(ratings.at[0, 0, step, some], tiles.at[some], scratch[1].at[g]).wait()
        place(g)


def slot_group(slots):
    return 8 if slots % 8 == 0 else 1


def in_hbm(*arrays):
    return [pltpu.with_memory_space_constraint(array, pltpu.HBM) for array in arrays]


def dense_ratings(
    step, tiles_per_shard, column_tiles, user_rows, tile_rows, tile_columns, tile_counts, ratings, fetched=False
):
    slots, tile = ratings.shape[3], ratings.shape[4]
    group = slot_group(slots)
    lists = (tile_counts, tile_rows, tile_columns)
    scratch = [pltpu.SMEM(some.shape, jnp.int32) for some in lists] + [pltpu.SemaphoreType.DMA((3,))]
    if not fetched:
        scratch = [
            pltpu.VMEM((slots, tile, tile), jnp.int32), pltpu.SemaphoreType.DMA((slots // group,)), *scratch
        ]
        operands, last_spec = in_hbm(*lists, ratings), HBM
    else:
        operands, last_spec = [*in_hbm(*lists), ratings], VMEM
    return pl.pallas_call(
        functools.partial(dense_kernel, step, tiles_per_shard, group, fetched),
        out_shape=jax.ShapeDtypeStruct((column_tiles, user_rows // tile, tile, tile), BF16),
        in_specs=[HBM] * 3 + [last_spec],
        out_specs=VMEM,
        scratch_shapes=scratch,
        compiler_params=pltpu.CompilerParams(vmem_limit_bytes=12 * MIB),
        cost_estimate=pl.CostEstimate(flops=2 * 10**9, bytes_accessed=8 * MIB, transcendentals=0),
    )(*operands)


def terms_kernel(columns, sizes, chunk, users_ref, users_t_ref, dense_ref, *refs):
    item_refs, (residual_ref, *grad_refs) = refs[: len(refs) - 1 - len(sizes)], refs[-1 - len(sizes) :]
    tile = dense_ref.shape[-1]
    per_chunk = chunk // tile
    items = jnp.concatenate([ref[...] for ref in item_refs], axis=0)
    chunks = users_ref.shape[0] // chunk

    def users(i):
        return users_ref[i * chunk : (i + 1) * chunk, :]

    def predict(i):
        users_t = users_t_ref[:, i * chunk : (i + 1) * chunk]
        return jnp.dot(items, users_t, preferred_element_type=F32)

    grad = None
    ahead = [predict(i) for i in range(min(LOOKAHEAD, chunks))]
    for i in range(chunks):
        predicted = ahead.pop(0)
        if i + LOOKAHEAD < chunks:
            ahead.append(predict(i + LOOKAHEAD))
        residuals = []
        for q in range(per_chunk):
            r = i * per_chunk + q
            rating = jnp.concatenate([dense_ref[j, r] for j in columns], axis=0).astype(F32)
            residual = jnp.where(
                rating > 0, rating - predicted[:, q * tile : (q + 1) * tile], 0.0
            ).astype(BF16)
            residual_ref[r] = residual
            residuals.append(residual)
        part = jnp.dot(jnp.concatenate(residuals, axis=1), users(i), preferred_element_type=F32)
        grad = part if grad is None else grad + part
    start = 0
    for ref in grad_refs:
        ref[...] = grad[start : start + ref.shape[0]]
        start += ref.shape[0]


def terms(columns, sizes, lowered, dense, items, last):
    user_rows, width = lowered[0].shape
    tile = dense.shape[-1]
    rows = tile * len(columns)
    return pl.pallas_call(
        functools.partial(terms_kernel, columns, sizes, min(CHUNK_TILES * tile, user_rows)),
        out_shape=[jax.ShapeDtypeStruct((user_rows // tile, rows, tile), BF16)]
        + [jax.ShapeDtypeStruct((size, width), F32) for size in sizes],
        in_specs=[VMEM] * (3 + len(items)),
        out_specs=[VMEM] * (1 + len(sizes)),
        compiler_params=pltpu.CompilerParams(vmem_limit_bytes=16 * MIB),
        cost_estimate=pl.CostEstimate(
            flops=int(LATENCY_SCALES[last] * 4 * user_rows * rows * width), bytes_accessed=MIB, transcendentals=0
        ),
    )(*lowered, dense, *items)


def users_kernel(number, chunk, last, users_ref, *refs):
    item_refs, refs = refs[:number], refs[number:]
    items = jnp.concatenate([ref[...] for ref in item_refs], axis=0)
    tile = refs[0].shape[-1]
    copies = []
    if last:
        *residual_refs, out_hbm, out_ref, sent = refs
    else:
        *residual_refs, out_ref, low_ref, low_t_ref = refs
    for i in range(users_ref.shape[0] // chunk):
        rows = slice(i * chunk, (i + 1) * chunk)
        residual = jnp.concatenate(
            [
                jnp.concatenate([ref[r] for ref in residual_refs], axis=0)
                for r in range(i * chunk // tile, (i + 1) * chunk // tile)
            ],
            axis=1,
        )
        total = lax.dot_general(residual, items, BOTH_ROWS, preferred_element_type=F32)
        users = users_ref[rows, :]
        updated = users + 0.01 * (total - 0.05 * users)
        out_ref[rows, :] = updated
        if last:
            copies.append(pltpu.make_async_copy(out_ref.at[rows], out_hbm.at[rows], sent.at[i]))
            copies[-1].start()
        else:
            lower_users(updated, rows, low_ref, low_t_ref)
    for copy in copies:
        copy.wait()


def update_users(users, items, residuals, last):
    user_rows, width = users.shape
    tile = residuals[0].shape[-1]
    chunk = min((2 if last else 4) * tile, user_rows)
    item_rows = sum(block.shape[0] for block in items)
    full = jax.ShapeDtypeStruct(users.shape, F32)
    if last:
        out_shape, out_specs = [full], [HBM]
        scratch = [pltpu.VMEM(users.shape, F32), pltpu.SemaphoreType.DMA((user_rows // chunk,))]
    else:
        out_shape, out_specs, scratch = [full, *low_shapes(users)], [VMEM] * 3, []
    return pl.pallas_call(
        functools.partial(users_kernel, len(items), chunk, last),
        out_shape=out_shape,
        in_specs=[VMEM] * (1 + len(items) + len(residuals)),
        out_specs=out_specs,
        scratch_shapes=scratch,
        compiler_params=pltpu.CompilerParams(vmem_limit_bytes=12 * MIB),
        cost_estimate=pl.CostEstimate(
            flops=int(LATENCY_SCALES[last] * 2 * user_rows * item_rows * width), bytes_accessed=4 * MIB, transcendentals=0
        ),
        name="users",
    )(users, *items, *residuals)


def updated_items(items, grad):
    return items + 0.003 * (grad - 0.05 * items)


def after(value, *earlier):
    return lax.optimization_barrier((value, *earlier))[0]


def paired_shards(user_factors, item_factors, tile_rows, tile_columns, tile_counts, ratings):
    step_total, tile = ratings.shape[2], ratings.shape[-1]
    per_shard = item_factors.shape[0] // tile
    column_tiles = per_shard * lax.axis_size("users")
    parts_rows = [slice(h * tile, (h + 1) * tile) for h in range(per_shard)]
    low = item_factors.astype(BF16)
    users_now, items_now = user_factors, item_factors
    held = {0: [low], 1: [route(low, 0, 1)], 2: [route(low, 0, 2)]}
    mark = []

    def ratings_of(step):
        dense = dense_ratings(
            step, per_shard, column_tiles, user_factors.shape[0],
            after(tile_rows, *mark), tile_columns, tile_counts, ratings, step > 0,
        )
        mark[:] = [dense]
        return dense

    dense = ratings_of(0)
    lowered = lower(after(user_factors, dense), tile)
    mark[:] = lowered[:1]
    for step in range(step_total):
        last = step == step_total - 1
        items_in, residuals, sums = [], [], []

        def run(d, block, first=0):
            blocks = block if isinstance(block, list) else [block]
            sizes = tuple(some.shape[0] for some in blocks)
            columns = tuple(
                (d + i) * per_shard + first + k for i, size in enumerate(sizes) for k in range(size // tile)
            )
            residual, *grads = terms(
                columns, sizes, lowered, dense, [after(blocks[0], *mark), *blocks[1:]], last
            )
            mark[:] = grads[-1:]
            items_in.extend(blocks)
            residuals.append(residual)
            return grads

        def near():
            own, passed = run(0, [held[0][0], held[1][0]])
            return own + route(passed, 0, 1)

        if step == 0:
            near_sum = near()
        for p, block in enumerate(held[2]):
            first = p * block.shape[0] // tile
            shared = route(after(block, *mark), 0, 1)
            (passed,) = run(2, block, first)
            passed = route(passed, 0, 1)
            if step > 0 and p == len(held[2]) - 1:
                held[1] = [route(after(held[0][0], *mark), 0, 1)]
            for k in range(block.shape[0] // tile):
                h, rows = first + k, parts_rows[k]
                (own,) = run(3, shared[rows], h)
                own = lax.optimization_barrier(own + passed[rows])
                mark.append(own)
                sums.append(route(own, 0, 3))
        if step > 0:
            near_sum = near()
        blocks = list(items_in)
        blocks[0] = after(blocks[0], *mark)
        users_now, *lowered = update_users(users_now, blocks, residuals, last)
        if last:
            return users_now, updated_items(items_now, near_sum + jnp.concatenate(sums, axis=0))
        mark[:] = lowered[:1]
        dense = ratings_of(step + 1)
        parts, low_parts = [], []
        for h, rows in enumerate(parts_rows):
            base = updated_items(items_now[rows], after(near_sum, *parts)[rows])
            parts.append(lax.optimization_barrier(base) + 0.003 * sums[h])
            low_parts.append(parts[h].astype(BF16))
        held = {2: [route(low, 1, 2) for low in low_parts]}
        held[0] = [route(jnp.concatenate(low_parts, axis=0), 1, 0)]
        items_now = after(jnp.concatenate(parts, axis=0), *mark)
        items_now = route(items_now, 1, 0)


def gathered_shards(user_factors, item_factors, tile_rows, tile_columns, tile_counts, ratings):
    step_total, tile = ratings.shape[2], ratings.shape[-1]
    users_now, item_part = user_factors, item_factors
    for step in range(step_total):
        block = lax.all_gather(item_part.astype(BF16), "users", axis=0, tiled=True)
        column_tiles = block.shape[0] // tile
        dense = dense_ratings(
            step, 0, column_tiles, users_now.shape[0], tile_rows, tile_columns, tile_counts, ratings
        )
        lowered = lower(users_now, tile)
        residual, grad = terms(tuple(range(column_tiles)), block.shape[:1], lowered, dense, [block], True)
        grad_part = lax.psum_scatter(grad, "users", scatter_dimension=0, tiled=True)
        users_now = update_users(users_now, [block], [residual], True)[0]
        item_part = updated_items(item_part, grad_part)
        if step < step_total - 1:
            item_part = route(item_part, 1, 0)
    return users_now, item_part


def solution(mesh):
    placed = (
        P(("strata", "users"), None),
        P(("strata", "users"), None),
        P("strata", "users", None, None),
        P("strata", "users", None, None),
        P("strata", "users", None),
        P("strata", "users", None, None, None, None),
    )

    def shards(user_factors, item_factors, *lists):
        tile = lists[-1].shape[-1]
        paired = mesh.shape["users"] == 4 and item_factors.shape[0] % tile == 0
        body = paired_shards if paired else gathered_shards
        return body(user_factors, item_factors, *lists)

    return jax.shard_map(
        shards,
        mesh=mesh,
        in_specs=placed,
        out_specs=(P(("strata", "users"), None), P(("strata", "users"), None)),
        check_vma=False,
    )
```

```python
import functools

import jax
import jax.numpy as jnp
from jax import lax
from jax.experimental import pallas as pl
from jax.experimental.pallas import tpu as pltpu
from jax.sharding import PartitionSpec as P


F32 = jnp.float32
BF16 = jnp.bfloat16
VMEM = pl.BlockSpec(memory_space=pltpu.VMEM)
HBM = pl.BlockSpec(memory_space=pltpu.HBM)
BOTH_ROWS = (((0,), (0,)), ((), ()))
MIB = 1 << 20
CHUNK_TILES = 2
LOOKAHEAD = 2
LATENCY_SCALES = (1, 3)


def route(block, strata_shift, users_flip):
    strata, users = lax.axis_size("strata"), lax.axis_size("users")
    pairs = [
        (s * users + u, ((s + strata_shift) % strata) * users + (u ^ users_flip))
        for s in range(strata)
        for u in range(users)
    ]
    return lax.ppermute(block, ("strata", "users"), pairs)


def lower_users(users, rows, low_ref, low_t_ref):
    low = users.astype(BF16)
    low_ref[rows, :] = low
    low_t_ref[:, rows] = low.T


def low_shapes(users):
    return [jax.ShapeDtypeStruct(users.shape, BF16), jax.ShapeDtypeStruct(users.shape[::-1], BF16)]


def lower_kernel(chunk, users_ref, low_ref, low_t_ref):
    for i in range(users_ref.shape[0] // chunk):
        rows = slice(i * chunk, (i + 1) * chunk)
        lower_users(users_ref[rows, :], rows, low_ref, low_t_ref)


def lower(users, tile):
    return pl.pallas_call(
        functools.partial(lower_kernel, tile),
        out_shape=low_shapes(users),
        in_specs=[VMEM],
        out_specs=[VMEM] * 2,
        compiler_params=pltpu.CompilerParams(vmem_limit_bytes=8 * MIB),
        cost_estimate=pl.CostEstimate(flops=10**8, bytes_accessed=MIB, transcendentals=0),
        name="lower",
    )(users)


def rating_copies(ratings_hbm, step, tiles, arrived):
    group = tiles.shape[0] // arrived.shape[0]
    return [
        pltpu.make_async_copy(
            ratings_hbm.at[0, 0, step, pl.ds(g * group, group)],
            tiles.at[pl.ds(g * group, group)],
            arrived.at[g],
        )
        for g in range(arrived.shape[0])
    ]


def dense_kernel(step, tiles_per_shard, group, fetched, counts_hbm, rows_hbm, columns_hbm, ratings, dense_ref, *scratch):
    *lists, listed = scratch if fetched else scratch[2:]
    tiles = ratings.at[0, 0, step] if fetched else scratch[0]
    counts_ref, rows_ref, columns_ref = lists
    flip = lax.axis_index("users") * tiles_per_shard
    copies = [
        pltpu.make_async_copy(source, target, listed.at[k])
        for k, (source, target) in enumerate(zip((counts_hbm, rows_hbm, columns_hbm), lists))
    ]
    for copy in copies:
        copy.start()
    if not fetched:
        for copy in rating_copies(ratings, step, tiles, scratch[1]):
            copy.start()

    @pl.loop(0, dense_ref.shape[0])
    def _(j):
        dense_ref[j] = jnp.zeros(dense_ref.shape[1:], BF16)

    for copy in copies:
        copy.wait()
    count = counts_ref[0, 0, step]

    def place(g):
        @pl.when(g * group < count)
        def _():
            for k in range(group):
                m = g * group + k
                j = columns_ref[0, 0, step, m] ^ flip
                r = rows_ref[0, 0, step, m]
                rating = jnp.where(m < count, tiles[m], 0)
                dense_ref[j, r] = rating.astype(F32).astype(BF16).T

    @pl.loop(0, tiles.shape[0] // group)
    def _(g):
        if not fetched:
            some = pl.ds(g * group, group)
            pltpu.make_async_copy(ratings.at[0, 0, step, some], tiles.at[some], scratch[1].at[g]).wait()
        place(g)


def slot_group(slots):
    return 8 if slots % 8 == 0 else 1


def in_hbm(*arrays):
    return [pltpu.with_memory_space_constraint(array, pltpu.HBM) for array in arrays]


def dense_ratings(
    step, tiles_per_shard, column_tiles, user_rows, tile_rows, tile_columns, tile_counts, ratings, fetched=False
):
    slots, tile = ratings.shape[3], ratings.shape[4]
    group = slot_group(slots) * (2 if fetched and slots % 16 == 0 else 1)
    lists = (tile_counts, tile_rows, tile_columns)
    scratch = [pltpu.SMEM(some.shape, jnp.int32) for some in lists] + [pltpu.SemaphoreType.DMA((3,))]
    if not fetched:
        scratch = [
            pltpu.VMEM((slots, tile, tile), jnp.int32), pltpu.SemaphoreType.DMA((slots // group,)), *scratch
        ]
        operands, last_spec = in_hbm(*lists, ratings), HBM
    else:
        operands, last_spec = [*in_hbm(*lists), ratings], VMEM
    return pl.pallas_call(
        functools.partial(dense_kernel, step, tiles_per_shard, group, fetched),
        out_shape=jax.ShapeDtypeStruct((column_tiles, user_rows // tile, tile, tile), BF16),
        in_specs=[HBM] * 3 + [last_spec],
        out_specs=VMEM,
        scratch_shapes=scratch,
        compiler_params=pltpu.CompilerParams(vmem_limit_bytes=12 * MIB),
        cost_estimate=pl.CostEstimate(flops=2 * 10**9, bytes_accessed=8 * MIB, transcendentals=0),
    )(*operands)


def terms_kernel(columns, sizes, chunk, users_ref, users_t_ref, dense_ref, *refs):
    item_refs, (residual_ref, *grad_refs) = refs[: len(refs) - 1 - len(sizes)], refs[-1 - len(sizes) :]
    tile = dense_ref.shape[-1]
    per_chunk = chunk // tile
    items = jnp.concatenate([ref[...] for ref in item_refs], axis=0)
    chunks = users_ref.shape[0] // chunk

    def users(i):
        return users_ref[i * chunk : (i + 1) * chunk, :]

    def predict(i):
        users_t = users_t_ref[:, i * chunk : (i + 1) * chunk]
        return jnp.dot(items, users_t, preferred_element_type=F32)

    grad = None
    ahead = [predict(i) for i in range(min(LOOKAHEAD, chunks))]
    for i in range(chunks):
        predicted = ahead.pop(0)
        if i + LOOKAHEAD < chunks:
            ahead.append(predict(i + LOOKAHEAD))
        residuals = []
        for q in range(per_chunk):
            r = i * per_chunk + q
            rating = jnp.concatenate([dense_ref[j, r] for j in columns], axis=0).astype(F32)
            residual = jnp.where(
                rating > 0, rating - predicted[:, q * tile : (q + 1) * tile], 0.0
            ).astype(BF16)
            residual_ref[r] = residual
            residuals.append(residual)
        part = jnp.dot(jnp.concatenate(residuals, axis=1), users(i), preferred_element_type=F32)
        grad = part if grad is None else grad + part
    start = 0
    for ref in grad_refs:
        ref[...] = grad[start : start + ref.shape[0]]
        start += ref.shape[0]


def terms(columns, sizes, lowered, dense, items, last):
    user_rows, width = lowered[0].shape
    tile = dense.shape[-1]
    rows = tile * len(columns)
    return pl.pallas_call(
        functools.partial(terms_kernel, columns, sizes, min(CHUNK_TILES * tile, user_rows)),
        out_shape=[jax.ShapeDtypeStruct((user_rows // tile, rows, tile), BF16)]
        + [jax.ShapeDtypeStruct((size, width), F32) for size in sizes],
        in_specs=[VMEM] * (3 + len(items)),
        out_specs=[VMEM] * (1 + len(sizes)),
        compiler_params=pltpu.CompilerParams(vmem_limit_bytes=16 * MIB),
        cost_estimate=pl.CostEstimate(
            flops=int(LATENCY_SCALES[last] * 4 * user_rows * rows * width), bytes_accessed=MIB, transcendentals=0
        ),
    )(*lowered, dense, *items)


def users_kernel(number, chunk, last, users_ref, *refs):
    item_refs, refs = refs[:number], refs[number:]
    items = jnp.concatenate([ref[...] for ref in item_refs], axis=0)
    tile = refs[0].shape[-1]
    copies = []
    if last:
        *residual_refs, out_hbm, out_ref, sent = refs
    else:
        *residual_refs, out_ref, low_ref, low_t_ref = refs
    for i in range(users_ref.shape[0] // chunk):
        rows = slice(i * chunk, (i + 1) * chunk)
        residual = jnp.concatenate(
            [
                jnp.concatenate([ref[r] for ref in residual_refs], axis=0)
                for r in range(i * chunk // tile, (i + 1) * chunk // tile)
            ],
            axis=1,
        )
        total = lax.dot_general(residual, items, BOTH_ROWS, preferred_element_type=F32)
        users = users_ref[rows, :]
        updated = users + 0.01 * (total - 0.05 * users)
        out_ref[rows, :] = updated
        if last:
            copies.append(pltpu.make_async_copy(out_ref.at[rows], out_hbm.at[rows], sent.at[i]))
            copies[-1].start()
        else:
            lower_users(updated, rows, low_ref, low_t_ref)
    for copy in copies:
        copy.wait()


def update_users(users, items, residuals, last):
    user_rows, width = users.shape
    tile = residuals[0].shape[-1]
    chunk = min((1 if last else 4) * tile, user_rows)
    item_rows = sum(block.shape[0] for block in items)
    full = jax.ShapeDtypeStruct(users.shape, F32)
    if last:
        out_shape, out_specs = [full], [HBM]
        scratch = [pltpu.VMEM(users.shape, F32), pltpu.SemaphoreType.DMA((user_rows // chunk,))]
    else:
        out_shape, out_specs, scratch = [full, *low_shapes(users)], [VMEM] * 3, []
    return pl.pallas_call(
        functools.partial(users_kernel, len(items), chunk, last),
        out_shape=out_shape,
        in_specs=[VMEM] * (1 + len(items) + len(residuals)),
        out_specs=out_specs,
        scratch_shapes=scratch,
        compiler_params=pltpu.CompilerParams(vmem_limit_bytes=12 * MIB),
        cost_estimate=pl.CostEstimate(
            flops=int(LATENCY_SCALES[last] * 2 * user_rows * item_rows * width), bytes_accessed=4 * MIB, transcendentals=0
        ),
        name="users",
    )(users, *items, *residuals)


def updated_items(items, grad):
    return items + 0.003 * (grad - 0.05 * items)


def after(value, *earlier):
    return lax.optimization_barrier((value, *earlier))[0]


def paired_shards(user_factors, item_factors, tile_rows, tile_columns, tile_counts, ratings):
    step_total, tile = ratings.shape[2], ratings.shape[-1]
    per_shard = item_factors.shape[0] // tile
    column_tiles = per_shard * lax.axis_size("users")
    parts_rows = [slice(h * tile, (h + 1) * tile) for h in range(per_shard)]
    low = item_factors.astype(BF16)
    users_now, items_now = user_factors, item_factors
    held = {0: [low], 1: [route(low, 0, 1)], 2: [route(low, 0, 2)]}
    mark = []

    def ratings_of(step):
        dense = dense_ratings(
            step, per_shard, column_tiles, user_factors.shape[0],
            after(tile_rows, *mark), tile_columns, tile_counts, ratings, step > 0,
        )
        mark[:] = [dense]
        return dense

    dense = ratings_of(0)
    lowered = lower(after(user_factors, dense), tile)
    mark[:] = lowered[:1]
    for step in range(step_total):
        last = step == step_total - 1
        items_in, residuals, sums = [], [], []

        def run(d, block, first=0):
            blocks = block if isinstance(block, list) else [block]
            sizes = tuple(some.shape[0] for some in blocks)
            columns = tuple(
                (d + i) * per_shard + first + k for i, size in enumerate(sizes) for k in range(size // tile)
            )
            residual, *grads = terms(
                columns, sizes, lowered, dense, [after(blocks[0], *mark), *blocks[1:]], last
            )
            mark[:] = grads[-1:]
            items_in.extend(blocks)
            residuals.append(residual)
            return grads

        def near():
            own, passed = run(0, [held[0][0], held[1][0]])
            return own + route(passed, 0, 1)

        if step == 0:
            near_sum = near()
        for p, block in enumerate(held[2]):
            first = p * block.shape[0] // tile
            shared = route(after(block, *mark), 0, 1)
            (passed,) = run(2, block, first)
            passed = route(passed, 0, 1)
            for k in range(block.shape[0] // tile):
                h, rows = first + k, parts_rows[k]
                (own,) = run(3, shared[rows], h)
                if step > 0 and h == per_shard - 1:
                    held[1] = [route(after(held[0][0], *mark), 0, 1)]
                own = lax.optimization_barrier(own + passed[rows])
                mark.append(own)
                sums.append(route(own, 0, 3))
        if step > 0:
            near_sum = near()
        blocks = list(items_in)
        blocks[0] = after(blocks[0], *mark)
        users_now, *lowered = update_users(users_now, blocks, residuals, last)
        if last:
            return users_now, updated_items(items_now, near_sum + jnp.concatenate(sums, axis=0))
        mark[:] = lowered[:1]
        dense = ratings_of(step + 1)
        parts, low_parts = [], []
        for h, rows in enumerate(parts_rows):
            base = updated_items(items_now[rows], after(near_sum, *parts)[rows])
            parts.append(lax.optimization_barrier(base) + 0.003 * sums[h])
            low_parts.append(parts[h].astype(BF16))
        held = {2: [route(low, 1, 2) for low in low_parts]}
        held[0] = [route(jnp.concatenate(low_parts, axis=0), 1, 0)]
        items_now = after(jnp.concatenate(parts, axis=0), *mark)
        items_now = route(items_now, 1, 0)


def gathered_shards(user_factors, item_factors, tile_rows, tile_columns, tile_counts, ratings):
    step_total, tile = ratings.shape[2], ratings.shape[-1]
    users_now, item_part = user_factors, item_factors
    for step in range(step_total):
        block = lax.all_gather(item_part.astype(BF16), "users", axis=0, tiled=True)
        column_tiles = block.shape[0] // tile
        dense = dense_ratings(
            step, 0, column_tiles, users_now.shape[0], tile_rows, tile_columns, tile_counts, ratings
        )
        lowered = lower(users_now, tile)
        residual, grad = terms(tuple(range(column_tiles)), block.shape[:1], lowered, dense, [block], True)
        grad_part = lax.psum_scatter(grad, "users", scatter_dimension=0, tiled=True)
        users_now = update_users(users_now, [block], [residual], True)[0]
        item_part = updated_items(item_part, grad_part)
        if step < step_total - 1:
            item_part = route(item_part, 1, 0)
    return users_now, item_part


def solution(mesh):
    placed = (
        P(("strata", "users"), None),
        P(("strata", "users"), None),
        P("strata", "users", None, None),
        P("strata", "users", None, None),
        P("strata", "users", None),
        P("strata", "users", None, None, None, None),
    )

    def shards(user_factors, item_factors, *lists):
        tile = lists[-1].shape[-1]
        per_shard, rest = divmod(item_factors.shape[0], tile)
        paired = mesh.shape["users"] == 4 and rest == 0 and per_shard.bit_count() == 1
        body = paired_shards if paired else gathered_shards
        return body(user_factors, item_factors, *lists)

    return jax.shard_map(
        shards,
        mesh=mesh,
        in_specs=placed,
        out_specs=(P(("strata", "users"), None), P(("strata", "users"), None)),
        check_vma=False,
    )
```
